32 devices in a mesh: member: 2 (over y), gy: 4 (over z), gx: 2 (over x), lev: 2 (over core).
Axes of the slice: x: 2, y: 2, z: 4, core: 2. Of those that a mesh axis runs over, the one named last changes fastest.
Arguments:
- level_field: bfloat16 [32, 1536, 1536], P(('member', 'lev'), 'gy', 'gx'), parts along dimension 0, may hold values from -6 to 6
Outputs:
- spectra: float32 [1536, 32, 1536], P(('gy', 'gx'), ('member', 'lev')), parts along dimension 1
- spectra_zone: float32 [1536, 32, 11], P(('gy', 'gx'), ('member', 'lev')), parts along dimension 1
The draws below stay inside these ranges and needn't reach their ends.
There are 2 independent parts, one for each index of `member`. The reference program is written for one: setup_inputs(seed, part) draws one part's arguments, and reference() takes and returns one part's arrays. A program takes and returns all parts, laid end to end along the dimension named above; each array names one. Nothing has to cross between parts.
All inputs are finite; a program needn't handle non-finite values.
Results may differ from the reference program's by a relative error of at most 0.0042.
Values may be sent and summed in bfloat16 or wider, within the bound.
A program may use at most 128 MiB of HBM per device.

```python
import math
import jax
import jax.numpy as jnp
from jax import lax

NX = 1536
NY = 1536
EXT_ZONE = 11
WAVES = 768
LEVELS = 16


def shard_levels(own_key, shape, cuts, low, largest):
    gain, own = 1.0, jax.random.fold_in(own_key, 6)
    for axis_at, parts in cuts:
        draws = jnp.exp(jax.random.uniform(jax.random.fold_in(own, axis_at), (parts,), jnp.float32, low / len(cuts), largest / len(cuts)))
        gain = gain * jnp.repeat(draws, shape[axis_at] // parts).reshape([-1 if axis == axis_at else 1 for axis in range(len(shape))])
    return gain


def centred(stream_key, dims, deviation, most, split=(), kind=jnp.bfloat16):
    drawn = deviation * jax.random.normal(stream_key, dims, jnp.float32)
    if split:
        drawn = drawn * shard_levels(stream_key, dims, split, -0.22, 0.18)
    return jnp.clip(drawn, -most, most).astype(kind)


def setup_inputs(seed: int = 0, part: int = 0) -> dict:
    keys = jax.random.split(jax.random.key(seed), 2)
    part_splits = jax.random.split(jax.random.fold_in(keys[1], part), 2)
    return {
        "level_field": centred(part_splits[0], (LEVELS, NY, NX), 1.0, 6.0, ((0, 2), (1, 4), (2, 2))),
    }


def blend_zone(second_last, last_value, first_value, second_value, zone_count):
    steps = (jnp.arange(zone_count, dtype=jnp.int32) + 1).astype(jnp.float32) / (zone_count + 1.0)
    weight_a = 2.0 * steps ** 3 - 3.0 * steps ** 2 + 1.0
    weight_b = steps ** 3 - 2.0 * steps ** 2 + steps
    weight_c = -2.0 * steps ** 3 + 3.0 * steps ** 2
    weight_d = steps ** 3 - steps ** 2
    tangent_scale = zone_count + 1.0
    slope_start = tangent_scale * (last_value - second_last)
    slope_end = tangent_scale * (second_value - first_value)
    return last_value[..., None] * weight_a + slope_start[..., None] * weight_b + first_value[..., None] * weight_c + slope_end[..., None] * weight_d

def make_table(wave_count, length):
    coeff = jnp.arange(2 * wave_count, dtype=jnp.int32)[:, None]
    column = jnp.arange(length, dtype=jnp.int32)[None, :]
    is_cosine = coeff < wave_count
    number = jnp.where(is_cosine, coeff, coeff - wave_count + 1)
    phase = (number * column % length).astype(jnp.float32) * (2.0 * math.pi / length)
    values = jnp.where(is_cosine, jnp.cos(phase), -jnp.sin(phase)) / math.sqrt(length)
    return values.astype(jnp.bfloat16)

def reference(level_field):
    widened = level_field.astype(jnp.float32)
    zone_x = blend_zone(widened[..., NX - 2], widened[..., NX - 1], widened[..., 0], widened[..., 1], EXT_ZONE).astype(jnp.bfloat16)
    extended = jnp.concatenate([level_field, zone_x], axis=2)
    wave_table = make_table(WAVES, NX + EXT_ZONE)

    def one_level(level_rows):
        return lax.dot_general(wave_table, level_rows, (((1,), (1,)), ((), ())), preferred_element_type=jnp.float32)
    stacked = lax.map(one_level, extended)
    spectra = jnp.transpose(stacked, (1, 0, 2))
    spectra_zone = blend_zone(spectra[..., NY - 2], spectra[..., NY - 1], spectra[..., 0], spectra[..., 1], EXT_ZONE)
    return (spectra, spectra_zone)
```

```python
import functools
import math

import jax
import jax.numpy as jnp
from jax import lax
from jax.experimental import pallas as pl
from jax.experimental.pallas import tpu as pltpu
from jax.sharding import PartitionSpec as P

EXT_ZONE = 11
LANES = 128
NT = (((1,), (1,)), ((), ()))
MESH = pl.DeviceIdType.MESH


def blend_weights(zone_count):
    steps = (jnp.arange(zone_count, dtype=jnp.int32) + 1).astype(jnp.float32) / (zone_count + 1.0)
    weight_a = 2.0 * steps**3 - 3.0 * steps**2 + 1.0
    weight_b = steps**3 - 2.0 * steps**2 + steps
    weight_c = -2.0 * steps**3 + 3.0 * steps**2
    weight_d = steps**3 - steps**2
    return weight_a, weight_b, weight_c, weight_d


def blend_zone(second_last, last_value, first_value, second_value, zone_count):
    weight_a, weight_b, weight_c, weight_d = blend_weights(zone_count)
    tangent_scale = zone_count + 1.0
    slope_start = tangent_scale * (last_value - second_last)
    slope_end = tangent_scale * (second_value - first_value)
    return (
        last_value[..., None] * weight_a
        + slope_start[..., None] * weight_b
        + first_value[..., None] * weight_c
        + slope_end[..., None] * weight_d
    )


def wave_factors(coeff0, group, column, wave_count, length):
    number0 = jnp.where(coeff0 < wave_count, coeff0, coeff0 - wave_count + 1)
    scale = 2.0 * math.pi / length
    phase0 = (number0[:, None] * column[None, :] % length).astype(jnp.float32) * scale
    cos0, sin0 = jnp.cos(phase0), jnp.sin(phase0)
    is_cosine = (coeff0 < wave_count)[:, None]
    p, q = jnp.where(is_cosine, cos0, -sin0), jnp.where(is_cosine, sin0, cos0)
    step = jnp.arange(group, dtype=jnp.int32)
    phase = (step[:, None] * column[None, :] % length).astype(jnp.float32) * scale
    norm = 1.0 / math.sqrt(length)
    return p, q, jnp.cos(phase) * norm, jnp.sin(phase) * norm


def kernel(n_gx, n_gy, field_ref, edge_ref, table_ref, ztable_ref, weight_ref,
           out_ref, out_edge_ref, xgot, xedge, send, esend, xs, xr, es, er, zs, zr, ts, tr):
    levels, rows, cols = field_ref.shape
    bands = table_ref.shape[2]
    me_x, me_y = lax.axis_index("gx"), lax.axis_index("gy")

    def peer_x(shift):
        return {"gx": lax.rem(me_x + n_gx - shift, n_gx)}

    def peer_y(shift):
        return {"gy": lax.rem(me_y + shift, n_gy)}

    barrier = pltpu.get_barrier_semaphore()
    for shift in range(1, n_gx):
        pl.semaphore_signal(barrier, inc=1, device_id=peer_x(shift), device_id_type=MESH)
    for shift in range(1, n_gy):
        pl.semaphore_signal(barrier, inc=1, device_id=peer_y(shift), device_id_type=MESH)
    pl.semaphore_wait(barrier, n_gx + n_gy - 2)

    def edge_x(shift):
        return pltpu.make_async_remote_copy(
            src_ref=edge_ref, dst_ref=xedge.at[shift - 1], send_sem=es.at[shift - 1],
            recv_sem=er.at[shift - 1], device_id=peer_x(shift), device_id_type=MESH)

    def rows_x(shift, level):
        return pltpu.make_async_remote_copy(
            src_ref=field_ref.at[level], dst_ref=xgot.at[shift - 1, level],
            send_sem=xs.at[shift - 1, level], recv_sem=xr.at[shift - 1, level],
            device_id=peer_x(shift), device_id_type=MESH)

    def edge_y(shift):
        return pltpu.make_async_remote_copy(
            src_ref=esend.at[shift - 1], dst_ref=out_edge_ref.at[shift], send_sem=ts.at[shift - 1],
            recv_sem=tr.at[shift - 1], device_id=peer_y(shift), device_id_type=MESH)

    def spec_y(shift, level):
        return pltpu.make_async_remote_copy(
            src_ref=send.at[shift - 1, level], dst_ref=out_ref.at[shift, level],
            send_sem=zs.at[shift - 1, level], recv_sem=zr.at[shift - 1, level],
            device_id=peer_y(shift), device_id_type=MESH)

    for shift in range(1, n_gx):
        edge_x(shift).start()

    @pl.loop(0, levels)
    def _(level):
        for shift in range(1, n_gx):
            rows_x(shift, level).start()

    tail = (cols - 1) // LANES * LANES

    def zone_of(parts):
        first = second = last = before = 0.0
        for at, part in enumerate(parts):
            owner = lax.rem(me_x + at, n_gx)
            is_first = jnp.where(owner == 0, 1.0, 0.0)
            is_last = jnp.where(owner == n_gx - 1, 1.0, 0.0)
            head = part[:, :min(LANES, cols)].astype(jnp.float32)
            rear = part[:, tail:].astype(jnp.float32)
            first += is_first * head[:, 0:1]
            second += is_first * head[:, 1:2]
            before += is_last * rear[:, cols - 2 - tail:cols - 1 - tail]
            last += is_last * rear[:, cols - 1 - tail:cols - tail]
        tangent = EXT_ZONE + 1.0
        zone = (last * weight_ref[0:1, :] + (tangent * (last - before)) * weight_ref[1:2, :]
                + first * weight_ref[2:3, :] + (tangent * (second - first)) * weight_ref[3:4, :])
        return zone.astype(jnp.bfloat16)

    def dot(a, b):
        return lax.dot_general(a, b, NT, preferred_element_type=jnp.float32)

    for shift in range(1, n_gx):
        edge_x(shift).wait_recv()
    parts = [edge_ref[...]] + [xedge[at] for at in range(n_gx - 1)]
    zone = zone_of(parts)
    for shift in range(n_gy):
        total = dot(zone, ztable_ref[shift])
        for at, part in enumerate(parts):
            total += dot(part, table_ref[at, shift])
        if shift == 0:
            out_edge_ref[0] = total
        else:
            esend[shift - 1] = total
            edge_y(shift).start()

    merged = bands % 16 == 0

    @pl.loop(0, levels)
    def _(level):
        for shift in range(1, n_gx):
            rows_x(shift, level).wait_recv()
        parts = [field_ref[level]] + [xgot[at, level] for at in range(n_gx - 1)]
        zone = zone_of(parts)
        if merged:
            size = n_gy * bands
            total = dot(ztable_ref[...].reshape(size, LANES), zone)
            for at, part in enumerate(parts):
                total += dot(table_ref[at].reshape(size, cols), part)
            pieces = [total[s * bands:(s + 1) * bands] for s in range(n_gy)]
        else:
            pieces = []
            for shift in range(n_gy):
                total = dot(ztable_ref[shift], zone)
                for at, part in enumerate(parts):
                    total += dot(table_ref[at, shift], part)
                pieces.append(total)
        for shift in range(n_gy):
            piece = pieces[shift].astype(jnp.bfloat16)
            if shift == 0:
                out_ref[0, level] = piece
            else:
                send[shift - 1, level] = piece
        for shift in range(1, n_gy):
            spec_y(shift, level).start()

    for shift in range(1, n_gx):
        edge_x(shift).wait_send()
    for shift in range(1, n_gy):
        edge_y(shift).wait()

    @pl.loop(0, levels)
    def _(level):
        for shift in range(1, n_gx):
            rows_x(shift, level).wait_send()
        for shift in range(1, n_gy):
            spec_y(shift, level).wait()


def make_body(mesh):
    n_gx, n_gy = mesh.shape["gx"], mesh.shape["gy"]

    def body(field):
        levels, rows, cols = field.shape
        nx, ny = cols * n_gx, rows * n_gy
        length = nx + EXT_ZONE
        me_x, me_y = lax.axis_index("gx"), lax.axis_index("gy")
        bands = nx // (n_gx * n_gy)
        assert (nx // 2) % bands == 0
        group = 16 if bands % 16 == 0 else bands

        at = jnp.arange(nx + LANES, dtype=jnp.int32)
        column = jnp.where(at < nx, (at + me_x * cols) % nx, at)
        shift_at = jnp.arange(n_gy, dtype=jnp.int32)[:, None]
        coeff = ((me_y + shift_at) % n_gy) * (n_gx * bands) + me_x * bands
        coeff = (coeff + jnp.arange(0, bands, group, dtype=jnp.int32)[None, :]).reshape(-1)
        factors = wave_factors(coeff, group, column, nx // 2, length)
        p, q, c, s = lax.optimization_barrier(factors)

        def expand(lo, hi):
            full = p[:, None, lo:hi] * c[None, :, lo:hi] - q[:, None, lo:hi] * s[None, :, lo:hi]
            return full.astype(jnp.bfloat16).reshape(n_gy, bands, hi - lo)

        table = jnp.stack([expand(i * cols, (i + 1) * cols) for i in range(n_gx)])
        ztable = expand(nx, nx + LANES)
        ztable = jnp.where(jnp.arange(LANES) < EXT_ZONE, ztable, jnp.zeros_like(ztable))
        weights = jnp.pad(jnp.stack(blend_weights(EXT_ZONE)), ((0, 4), (0, LANES - EXT_ZONE)))
        edge = jnp.concatenate([field[:, :2], field[:, rows - 2:]], axis=1)
        edge = edge.transpose(1, 0, 2).reshape(4 * levels, cols)

        vmem = pl.BlockSpec(memory_space=pltpu.VMEM)
        dma = pltpu.SemaphoreType.DMA
        xs, ys = n_gx - 1, n_gy - 1
        got, edge_got = pl.pallas_call(
            functools.partial(kernel, n_gx, n_gy),
            out_shape=(
                jax.ShapeDtypeStruct((n_gy, levels, bands, rows), jnp.bfloat16),
                jax.ShapeDtypeStruct((n_gy, 4 * levels, bands), jnp.float32),
            ),
            in_specs=[vmem] * 5,
            out_specs=(vmem, vmem),
            scratch_shapes=[
                pltpu.VMEM((xs, levels, rows, cols), jnp.bfloat16),
                pltpu.VMEM((xs, 4 * levels, cols), jnp.bfloat16),
                pltpu.VMEM((ys, levels, bands, rows), jnp.bfloat16),
                pltpu.VMEM((ys, 4 * levels, bands), jnp.float32),
                dma((xs, levels)), dma((xs, levels)), dma((xs,)), dma((xs,)),
                dma((ys, levels)), dma((ys, levels)), dma((ys,)), dma((ys,)),
            ],
            compiler_params=pltpu.CompilerParams(collective_id=0, has_side_effects=True),
        )(field, edge, table, ztable, weights)

        edge_got = edge_got.reshape(n_gy, 4, levels, bands)
        low = lax.dynamic_index_in_dim(edge_got, me_y, 0, keepdims=False)
        high = lax.dynamic_index_in_dim(edge_got, (me_y + 1) % n_gy, 0, keepdims=False)
        low, high = low.transpose(0, 2, 1), high.transpose(0, 2, 1)
        spectra_zone = blend_zone(high[2], high[3], low[0], low[1], EXT_ZONE)

        spectra = jnp.zeros((bands, levels, ny), jnp.float32)
        for shift in range(n_gy):
            full = got[shift].transpose(1, 0, 2).astype(jnp.float32)
            source = (me_y + n_gy - shift) % n_gy
            spectra = lax.dynamic_update_slice(spectra, full, (0, 0, source * rows))
        return spectra, spectra_zone

    return body


def solution(mesh):
    return jax.shard_map(
        make_body(mesh),
        mesh=mesh,
        in_specs=(P(("member", "lev"), "gy", "gx"),),
        out_specs=(
            P(("gy", "gx"), ("member", "lev"), None),
            P(("gy", "gx"), ("member", "lev"), None),
        ),
        check_vma=False,
    )
```

```python
import functools
import math

import jax
import jax.numpy as jnp
from jax import lax
from jax.experimental import pallas as pl
from jax.experimental.pallas import tpu as pltpu
from jax.sharding import PartitionSpec as P

EXT_ZONE = 11
LANES = 128
NT = (((1,), (1,)), ((), ()))
MESH = pl.DeviceIdType.MESH


def blend_weights(zone_count):
    steps = (jnp.arange(zone_count, dtype=jnp.int32) + 1).astype(jnp.float32) / (zone_count + 1.0)
    weight_a = 2.0 * steps**3 - 3.0 * steps**2 + 1.0
    weight_b = steps**3 - 2.0 * steps**2 + steps
    weight_c = -2.0 * steps**3 + 3.0 * steps**2
    weight_d = steps**3 - steps**2
    return weight_a, weight_b, weight_c, weight_d


def blend_zone(second_last, last_value, first_value, second_value, zone_count):
    weight_a, weight_b, weight_c, weight_d = blend_weights(zone_count)
    tangent_scale = zone_count + 1.0
    slope_start = tangent_scale * (last_value - second_last)
    slope_end = tangent_scale * (second_value - first_value)
    return (
        last_value[..., None] * weight_a
        + slope_start[..., None] * weight_b
        + first_value[..., None] * weight_c
        + slope_end[..., None] * weight_d
    )


def wave_factors(coeff0, group, column, wave_count, length):
    number0 = jnp.where(coeff0 < wave_count, coeff0, coeff0 - wave_count + 1)
    scale = 2.0 * math.pi / length
    phase0 = (number0[:, None] * column[None, :] % length).astype(jnp.float32) * scale
    cos0, sin0 = jnp.cos(phase0), jnp.sin(phase0)
    is_cosine = (coeff0 < wave_count)[:, None]
    p, q = jnp.where(is_cosine, cos0, -sin0), jnp.where(is_cosine, sin0, cos0)
    step = jnp.arange(group, dtype=jnp.int32)
    phase = (step[:, None] * column[None, :] % length).astype(jnp.float32) * scale
    norm = 1.0 / math.sqrt(length)
    return p, q, jnp.cos(phase) * norm, jnp.sin(phase) * norm


def kernel(n_gx, n_gy, field_ref, edge_ref, table_ref, ztable_ref, weight_ref,
           out_ref, out_edge_ref, xgot, xedge, send, esend, xs, xr, es, er, zs, zr, ts, tr):
    levels, rows, cols = field_ref.shape
    bands = table_ref.shape[2]
    me_x, me_y = lax.axis_index("gx"), lax.axis_index("gy")

    def peer_x(shift):
        return {"gx": lax.rem(me_x + n_gx - shift, n_gx)}

    def peer_y(shift):
        return {"gy": lax.rem(me_y + shift, n_gy)}

    barrier = pltpu.get_barrier_semaphore()
    for shift in range(1, n_gx):
        pl.semaphore_signal(barrier, inc=1, device_id=peer_x(shift), device_id_type=MESH)
    for shift in range(1, n_gy):
        pl.semaphore_signal(barrier, inc=1, device_id=peer_y(shift), device_id_type=MESH)
    pl.semaphore_wait(barrier, n_gx + n_gy - 2)

    def edge_x(shift):
        return pltpu.make_async_remote_copy(
            src_ref=edge_ref, dst_ref=xedge.at[shift - 1], send_sem=es.at[shift - 1],
            recv_sem=er.at[shift - 1], device_id=peer_x(shift), device_id_type=MESH)

    def rows_x(shift, level):
        return pltpu.make_async_remote_copy(
            src_ref=field_ref.at[level], dst_ref=xgot.at[shift - 1, level],
            send_sem=xs.at[shift - 1, level], recv_sem=xr.at[shift - 1, level],
            device_id=peer_x(shift), device_id_type=MESH)

    def edge_y(shift):
        return pltpu.make_async_remote_copy(
            src_ref=esend.at[shift - 1], dst_ref=out_edge_ref.at[me_y], send_sem=ts.at[shift - 1],
            recv_sem=tr.at[shift - 1], device_id=peer_y(shift), device_id_type=MESH)

    def spec_y(shift, level):
        return pltpu.make_async_remote_copy(
            src_ref=send.at[shift - 1, level], dst_ref=out_ref.at[me_y, level],
            send_sem=zs.at[shift - 1, level], recv_sem=zr.at[shift - 1, level],
            device_id=peer_y(shift), device_id_type=MESH)

    for shift in range(1, n_gx):
        edge_x(shift).start()

    @pl.loop(0, levels)
    def _(level):
        for shift in range(1, n_gx):
            rows_x(shift, level).start()

    tail = (cols - 1) // LANES * LANES

    def zone_of(parts):
        first = second = last = before = 0.0
        for at, part in enumerate(parts):
            owner = lax.rem(me_x + at, n_gx)
            is_first = jnp.where(owner == 0, 1.0, 0.0)
            is_last = jnp.where(owner == n_gx - 1, 1.0, 0.0)
            head = part[:, :min(LANES, cols)].astype(jnp.float32)
            rear = part[:, tail:].astype(jnp.float32)
            first += is_first * head[:, 0:1]
            second += is_first * head[:, 1:2]
            before += is_last * rear[:, cols - 2 - tail:cols - 1 - tail]
            last += is_last * rear[:, cols - 1 - tail:cols - tail]
        tangent = EXT_ZONE + 1.0
        zone = (last * weight_ref[0:1, :] + (tangent * (last - before)) * weight_ref[1:2, :]
                + first * weight_ref[2:3, :] + (tangent * (second - first)) * weight_ref[3:4, :])
        return zone.astype(jnp.bfloat16)

    def dot(a, b):
        return lax.dot_general(a, b, NT, preferred_element_type=jnp.float32)

    for shift in range(1, n_gx):
        edge_x(shift).wait_recv()
    parts = [edge_ref[...]] + [xedge[at] for at in range(n_gx - 1)]
    zone = zone_of(parts)
    for shift in range(n_gy):
        total = dot(zone, ztable_ref[shift])
        for at, part in enumerate(parts):
            total += dot(part, table_ref[at, shift])
        if shift == 0:
            out_edge_ref[me_y] = total
        else:
            esend[shift - 1] = total
            edge_y(shift).start()

    merged = bands % 16 == 0

    @pl.loop(0, levels)
    def _(level):
        for shift in range(1, n_gx):
            rows_x(shift, level).wait_recv()
        parts = [field_ref[level]] + [xgot[at, level] for at in range(n_gx - 1)]
        zone = zone_of(parts)
        if merged:
            size = n_gy * bands
            total = dot(ztable_ref[...].reshape(size, LANES), zone)
            for at, part in enumerate(parts):
                total += dot(table_ref[at].reshape(size, cols), part)
            pieces = [total[s * bands:(s + 1) * bands] for s in range(n_gy)]
        else:
            pieces = []
            for shift in range(n_gy):
                total = dot(ztable_ref[shift], zone)
                for at, part in enumerate(parts):
                    total += dot(table_ref[at, shift], part)
                pieces.append(total)
        for shift in range(n_gy):
            piece = pieces[shift].astype(jnp.bfloat16)
            if shift == 0:
                out_ref[me_y, level] = piece
            else:
                send[shift - 1, level] = piece
        for shift in range(1, n_gy):
            spec_y(shift, level).start()

    for shift in range(1, n_gx):
        edge_x(shift).wait_send()
    for shift in range(1, n_gy):
        edge_y(shift).wait()

    @pl.loop(0, levels)
    def _(level):
        for shift in range(1, n_gx):
            rows_x(shift, level).wait_send()
        for shift in range(1, n_gy):
            spec_y(shift, level).wait()


def make_body(mesh):
    n_gx, n_gy = mesh.shape["gx"], mesh.shape["gy"]

    def body(field):
        levels, rows, cols = field.shape
        nx, ny = cols * n_gx, rows * n_gy
        length = nx + EXT_ZONE
        me_x, me_y = lax.axis_index("gx"), lax.axis_index("gy")
        bands = nx // (n_gx * n_gy)
        assert (nx // 2) % bands == 0
        group = 16 if bands % 16 == 0 else bands

        at = jnp.arange(nx + LANES, dtype=jnp.int32)
        column = jnp.where(at < nx, (at + me_x * cols) % nx, at)
        shift_at = jnp.arange(n_gy, dtype=jnp.int32)[:, None]
        coeff = ((me_y + shift_at) % n_gy) * (n_gx * bands) + me_x * bands
        coeff = (coeff + jnp.arange(0, bands, group, dtype=jnp.int32)[None, :]).reshape(-1)
        factors = wave_factors(coeff, group, column, nx // 2, length)
        p, q, c, s = lax.optimization_barrier(factors)

        def expand(lo, hi):
            full = p[:, None, lo:hi] * c[None, :, lo:hi] - q[:, None, lo:hi] * s[None, :, lo:hi]
            return full.astype(jnp.bfloat16).reshape(n_gy, bands, hi - lo)

        table = jnp.stack([expand(i * cols, (i + 1) * cols) for i in range(n_gx)])
        ztable = expand(nx, nx + LANES)
        ztable = jnp.where(jnp.arange(LANES) < EXT_ZONE, ztable, jnp.zeros_like(ztable))
        weights = jnp.pad(jnp.stack(blend_weights(EXT_ZONE)), ((0, 4), (0, LANES - EXT_ZONE)))
        edge = jnp.concatenate([field[:, :2], field[:, rows - 2:]], axis=1)
        edge = edge.transpose(1, 0, 2).reshape(4 * levels, cols)

        vmem = pl.BlockSpec(memory_space=pltpu.VMEM)
        dma = pltpu.SemaphoreType.DMA
        xs, ys = n_gx - 1, n_gy - 1
        got, edge_got = pl.pallas_call(
            functools.partial(kernel, n_gx, n_gy),
            out_shape=(
                jax.ShapeDtypeStruct((n_gy, levels, bands, rows), jnp.bfloat16),
                jax.ShapeDtypeStruct((n_gy, 4 * levels, bands), jnp.float32),
            ),
            in_specs=[vmem] * 5,
            out_specs=(vmem, vmem),
            scratch_shapes=[
                pltpu.VMEM((xs, levels, rows, cols), jnp.bfloat16),
                pltpu.VMEM((xs, 4 * levels, cols), jnp.bfloat16),
                pltpu.VMEM((ys, levels, bands, rows), jnp.bfloat16),
                pltpu.VMEM((ys, 4 * levels, bands), jnp.float32),
                dma((xs, levels)), dma((xs, levels)), dma((xs,)), dma((xs,)),
                dma((ys, levels)), dma((ys, levels)), dma((ys,)), dma((ys,)),
            ],
            compiler_params=pltpu.CompilerParams(collective_id=0, has_side_effects=True),
        )(field, edge, table, ztable, weights)

        edge_got = edge_got.reshape(n_gy, 4, levels, bands)
        low, high = edge_got[0], edge_got[n_gy - 1]
        low, high = low.transpose(0, 2, 1), high.transpose(0, 2, 1)
        spectra_zone = blend_zone(high[2], high[3], low[0], low[1], EXT_ZONE)

        spectra = got.transpose(2, 1, 0, 3).reshape(bands, levels, ny).astype(jnp.float32)
        return spectra, spectra_zone

    return body


def solution(mesh):
    return jax.shard_map(
        make_body(mesh),
        mesh=mesh,
        in_specs=(P(("member", "lev"), "gy", "gx"),),
        out_specs=(
            P(("gy", "gx"), ("member", "lev"), None),
            P(("gy", "gx"), ("member", "lev"), None),
        ),
        check_vma=False,
    )
```
